32 devices in a mesh: batch: 4 (over x, core), seq: 8 (over z, y).
Axes of the slice: x: 2, y: 2, z: 4, core: 2. Of those that a mesh axis runs over, the one named last changes fastest.
Arguments:
- layer_inputs: bfloat16 [25600, 800], P(('batch', 'seq')), may hold values from -24 to 24
- output_grads: bfloat16 [25600, 800], P(('batch', 'seq')), may hold values from -48 to 48
- input_inverse: float32 [800, 200], replicated, may hold values from -1 to 3
- output_inverse: float32 [800, 200], replicated, may hold values from -1 to 3
Outputs:
- input_factor: float32 [800, 200], P('seq')
- output_factor: float32 [800, 200], P('seq')
- preconditioned: bfloat16 [800, 800], replicated
The draws below stay inside these ranges and needn't reach their ends.
All inputs are finite; a program needn't handle non-finite values.
Results may differ from the reference program's by a relative error of at most 0.0075.
Values may be sent and summed in bfloat16 or wider, within the bound.
A program may use at most 64 MiB of HBM per device.

```python
import math
import jax
import jax.numpy as jnp
from jax import lax

DIN = 800
DOUT = 800
BLOCK = 200
TOK_DEV = 800
TOKENS = 25600


def shared_latent(key):
    return jax.random.normal(jax.random.fold_in(key, 11), (TOKENS, BLOCK), jnp.float32)


def mixed_draw(key, width, salt, strength, limit):
    latent = shared_latent(key)
    mixing = jax.random.normal(jax.random.fold_in(key, salt), (BLOCK, width), jnp.float32) * (strength / math.sqrt(BLOCK))
    noise_key = jax.random.fold_in(key, salt + 1)
    noise = jax.random.normal(noise_key, (TOKENS, width), jnp.float32)
    row_ids = jnp.arange(TOKENS, dtype=jnp.int32)
    device = row_ids // TOK_DEV
    rising = 1.0 + 2.0 * row_ids.astype(jnp.float32) / TOKENS
    offset = jax.random.randint(jax.random.fold_in(key, salt + 3), (), 0, 32, jnp.int32)
    group = jnp.arange(width, dtype=jnp.int32) // (width // 32)
    spiked = (device[:, None] + offset) % 32 == group[None, :]
    boost = jnp.where(spiked, 3.0, 1.0)
    values = 0.6 * noise * rising[:, None] * boost + jnp.dot(latent, mixing)
    return jnp.clip(values, -limit, limit)


def draw_layer_inputs(key, part):
    return mixed_draw(key, DIN, 101, 1.0, 24.0).astype(jnp.bfloat16)


def draw_output_grads(key, part):
    return mixed_draw(key, DOUT, 201, 3.0, 48.0).astype(jnp.bfloat16)


def inverse_blocks(key, width):
    count = width // BLOCK
    noise_key = jax.random.fold_in(key, 301)
    noise = jax.random.normal(noise_key, (count, BLOCK, BLOCK), jnp.float32)
    symmetric = (noise + jnp.swapaxes(noise, 1, 2)) * (0.4 / math.sqrt(2.0 * BLOCK))
    diagonal = jnp.exp(jax.random.uniform(jax.random.fold_in(key, 302), (count, BLOCK), jnp.float32, math.log(0.5), math.log(2.0)))
    matrix = symmetric + jnp.eye(BLOCK, dtype=jnp.float32)[None, :, :] * diagonal[:, :, None]
    return jnp.clip(matrix, -1.0, 3.0).reshape(width, BLOCK)


def draw_input_inverse(key, part):
    return inverse_blocks(jax.random.fold_in(key, 401), DIN)


def draw_output_inverse(key, part):
    return inverse_blocks(jax.random.fold_in(key, 402), DOUT)


def setup_inputs(seed: int = 0) -> dict:
    key_of = jax.random.split(jax.random.key(seed), 5)
    return {
        "layer_inputs": draw_layer_inputs(jax.random.fold_in(key_of[4], 71), 0),
        "output_grads": draw_output_grads(jax.random.fold_in(key_of[4], 71), 0),
        "input_inverse": draw_input_inverse(jax.random.fold_in(key_of[4], 71), 0),
        "output_inverse": draw_output_inverse(jax.random.fold_in(key_of[4], 71), 0),
    }


def block_covariance(values):
    width = values.shape[1]
    products = []
    for number in range(width // BLOCK):
        columns = values[:, number * BLOCK:(number + 1) * BLOCK]
        products.append(jnp.dot(columns.T, columns, preferred_element_type=jnp.float32))
    return jnp.concatenate(products, axis=0)


def reference(layer_inputs, output_grads, input_inverse, output_inverse):
    inverse_count = 1.0 / TOKENS
    input_factor = block_covariance(layer_inputs) * inverse_count
    output_factor = block_covariance(output_grads) * inverse_count
    gradient = jnp.dot(layer_inputs.T, output_grads, preferred_element_type=jnp.float32) * inverse_count
    in_blocks = DIN // BLOCK
    out_blocks = DOUT // BLOCK
    right_side = jnp.einsum("imk,mkl->iml", gradient.reshape(DIN, out_blocks, BLOCK),
                            output_inverse.reshape(out_blocks, BLOCK, BLOCK),
                            precision=lax.Precision.HIGHEST).reshape(DIN, DOUT)
    applied = jnp.einsum("nij,njo->nio", input_inverse.reshape(in_blocks, BLOCK, BLOCK),
                         right_side.reshape(in_blocks, BLOCK, DOUT),
                         precision=lax.Precision.HIGHEST).reshape(DIN, DOUT)
    return input_factor, output_factor, applied.astype(jnp.bfloat16)
```

```python
import functools

import jax
import jax.numpy as jnp
from jax import lax
from jax.experimental import pallas as pl
from jax.experimental.pallas import tpu as pltpu
from jax.sharding import PartitionSpec as P

BLOCK = 200


def block_terms(values):
    tok_rows, width = values.shape
    stacked = values.reshape(tok_rows, width // BLOCK, BLOCK)
    product = jnp.einsum("tnb,tnc->nbc", stacked, stacked, preferred_element_type=jnp.float32)
    return product.reshape(width, BLOCK)


def reduce_terms(input_term, output_term, grad_term):
    shares = (
        lax.psum_scatter(
            input_term.astype(jnp.bfloat16), "seq", scatter_dimension=0, tiled=True
        ).astype(jnp.float32),
        lax.psum_scatter(
            output_term.astype(jnp.bfloat16), "seq", scatter_dimension=0, tiled=True
        ).astype(jnp.float32),
        lax.psum_scatter(
            grad_term.astype(jnp.bfloat16), "seq", scatter_dimension=0, tiled=True
        ).astype(jnp.float32),
    )
    return lax.psum((shares[0], shares[1], shares[2]), "batch")


def shards(layer_inputs, output_grads, input_inverse, output_inverse):
    tok_rows, in_width = layer_inputs.shape
    out_width = output_grads.shape[1]
    in_blocks = in_width // BLOCK
    out_blocks = out_width // BLOCK
    total_rows = tok_rows * lax.axis_size("batch") * lax.axis_size("seq")
    inverse_count = 1.0 / total_rows
    input_term = block_terms(layer_inputs)
    output_term = block_terms(output_grads)
    input_stack = input_inverse.reshape(in_blocks, BLOCK, BLOCK)
    output_stack = output_inverse.reshape(out_blocks, BLOCK, BLOCK)
    grad_term = lax.dot_general(
        layer_inputs, output_grads, (((0,), (0,)), ((), ())), preferred_element_type=jnp.float32
    )
    input_sum, output_sum, grad_sum = reduce_terms(input_term, output_term, grad_term)
    grad_owned = grad_sum * inverse_count
    owned_rows = grad_owned.shape[0]
    right_done = jnp.einsum(
        "rmk,mkl->rml",
        grad_owned.reshape(owned_rows, out_blocks, BLOCK),
        output_stack,
        precision=lax.Precision.HIGHEST,
    ).reshape(owned_rows, out_width)
    gathered = lax.all_gather(right_done, "seq", axis=0, tiled=True)
    applied = jnp.einsum(
        "nij,njo->nio",
        input_stack,
        gathered.reshape(in_blocks, BLOCK, out_width),
        precision=lax.Precision.HIGHEST,
    ).reshape(in_width, out_width)
    preconditioned = applied.astype(jnp.bfloat16)
    input_factor = input_sum * inverse_count
    output_factor = output_sum * inverse_count
    return (input_factor, output_factor, preconditioned)


LANE = 128
PAD = 2 * LANE
MESH = pl.DeviceIdType.MESH


def round_up(size, unit):
    return (size + unit - 1) // unit * unit


def kernel(
    near, x_hbm, y_hbm, pinv_hbm, qinv_hbm, fx_ref, fy_ref, out_ref,
    x_ref, y_ref, pinv_ref, qinv_ref, load_s, xp, yp, g_own, g_away, g_stage, g_core, x_send, x_recv, y_send, y_recv, z_send, z_recv,
    f_own, f_stage, f_core, fy_send, fy_recv, fz_send, fz_recv, fx_send, fx_recv, fc_send, fc_recv,
    gc_send, gc_recv, ag,
    core_s, core_r, x_s, x_r, y_s, y_r, z_s, z_r, fy_s, fy_r, fz_s, fz_r, fin_s, fin_r,
    az_s, az_r, ay_s, ay_r, ax_s, ax_r, ac_s, ac_r,
):
    batch, seq = lax.axis_index("batch"), lax.axis_index("seq")
    x, c = batch // 2, batch % 2
    z, y = seq // 2, seq % 2
    tok, in_width = x_hbm.shape
    out_width = y_hbm.shape[1]
    in_blocks, out_blocks = in_width // BLOCK, out_width // BLOCK
    half_in = in_blocks // 2
    rows = g_own.shape[1]
    per_x = half_in * out_blocks
    window, step = f_own.shape[2], rows - f_own.shape[2]
    scale = 1.0 / (tok * lax.axis_size("batch") * lax.axis_size("seq"))
    core_peer = (2 * x + 1 - c, seq)
    x_peer = (2 * (1 - x) + c, seq)
    y_peer = (batch, 2 * z + 1 - y)

    def z_peer(to):
        return (batch, 2 * to + y)

    def around(i):
        return lax.rem(z + i, near)

    def remote(src, dst, s, r, peer):
        return pltpu.make_async_remote_copy(
            src_ref=src, dst_ref=dst, send_sem=s, recv_sem=r, device_id=peer, device_id_type=MESH
        )

    pending = []

    def send(*args):
        copy = remote(*args)
        copy.start()
        pending.append(copy)
        return copy

    loads = [
        pltpu.make_async_copy(src, dst, load_s.at[i])
        for i, (src, dst) in enumerate(
            ((x_hbm, x_ref), (y_hbm, y_ref), (pinv_hbm, pinv_ref), (qinv_hbm, qinv_ref))
        )
    ]
    for load in loads:
        load.start()
    barrier = pltpu.get_barrier_semaphore()
    peers = [core_peer, x_peer, y_peer] + [z_peer(around(i)) for i in range(1, near)]
    for peer in peers:
        pl.semaphore_signal(barrier, inc=1, device_id=peer, device_id_type=MESH)

    def padded(ref, out, blocks):
        for b in range(blocks):
            part = ref[:, b * BLOCK:(b + 1) * BLOCK]
            out[:, b * PAD:b * PAD + BLOCK] = part
            out[:, b * PAD + BLOCK:(b + 1) * PAD] = jnp.zeros((tok, PAD - BLOCK), out.dtype)

    loads[0].wait()
    padded(x_ref, xp, in_blocks)
    loads[1].wait()
    padded(y_ref, yp, out_blocks)

    def tdot(a, b):
        return lax.dot_general(a, b, (((0,), (0,)), ((), ())), preferred_element_type=jnp.float32)

    first = c == 0
    f32 = jnp.float32

    def mine(v):
        return jnp.where(first, v[:, :LANE], v[:, LANE:PAD])

    def other(v):
        return jnp.where(first, v[:, LANE:PAD], v[:, :LANE])

    far, own = 1 - z // 2, z // 2
    owners = out_blocks // 2

    def grads(to_x, keep, strip, base):
        col = pl.multiple_of((half_in * to_x + strip) * PAD, PAD)
        prod = tdot(xp[:, pl.ds(col, PAD)], yp[...])[:rows]
        for m in range(out_blocks):
            k = strip * out_blocks + m
            part = prod[:, m * PAD:(m + 1) * PAD]
            keep[k] = mine(part)
            g_stage[base + k] = other(part).astype(jnp.bfloat16)

    def swap(base, count, i):
        return send(g_stage.at[pl.ds(base, count)], g_core.at[pl.ds(base, count)], core_s.at[i], core_r.at[i], core_peer)

    grads(1 - x, g_away, far, 0)
    pl.semaphore_wait(barrier, len(peers))
    core_a = swap(far * out_blocks, out_blocks, 0)
    grads(1 - x, g_away, own, 0)
    core_b = swap(own * out_blocks, out_blocks, 1)

    def to_x(strip, core):
        core.wait_recv()
        for yy in (1 - y, y):
            for j in range(owners):
                k = 2 * (strip * owners + j) + yy
                x_send[k] = (g_away[k] + g_core[k].astype(f32)).astype(jnp.bfloat16)
                send(x_send.at[k], x_recv.at[k], x_s.at[k], x_r.at[k], x_peer)

    to_x(far, core_a)

    def factors(j, src):
        for b in range(in_blocks):
            part = src[:, b * PAD:(b + 1) * PAD]
            prod = tdot(part, part)
            keep, away = mine(prod), other(prod)
            for h in range(2):
                f_own[2 * b + h, j] = keep[h * step:h * step + window]
                f_stage[2 * b + h, j] = away[h * step:h * step + window].astype(jnp.bfloat16)

    factors(0, xp)
    to_x(own, core_b)
    factors(1, yp)
    core_f = send(f_stage, f_core, core_s.at[2], core_r.at[2], core_peer)
    for strip in (far, own):
        grads(x, g_own, strip, per_x)
    core_c = swap(per_x, per_x, 3)

    order = [far * owners + j for j in range(owners)]
    order += [own * owners + (z + 1 + j) % owners for j in range(owners)]

    def got_x(k):
        remote(x_send.at[k], x_recv.at[k], x_s.at[k], x_r.at[k], x_peer).wait_recv()
        return g_own[k] + g_core[per_x + k].astype(f32) + x_recv[k].astype(f32)

    def grad_y(to):
        y_send[to] = got_x(2 * to + 1 - y).astype(jnp.bfloat16)
        send(y_send.at[to], y_recv.at[to], y_s.at[to], y_r.at[to], y_peer)

    def factor_y(to):
        k = 2 * to + 1 - y
        fy_send[to] = (f_own[k] + f_core[k].astype(f32)).astype(jnp.bfloat16)
        send(fy_send.at[to], fy_recv.at[to], fy_s.at[to], fy_r.at[to], y_peer)

    def got_factor(to):
        k = 2 * to + y
        remote(fy_send.at[to], fy_recv.at[to], fy_s.at[to], fy_r.at[to], y_peer).wait_recv()
        return f_own[k] + f_core[k].astype(f32) + fy_recv[to].astype(f32)

    def factor_z(to):
        fz_send[to] = got_factor(to).astype(jnp.bfloat16)
        send(fz_send.at[to], fz_recv.at[z], fz_s.at[to], fz_r.at[z], z_peer(to))

    def got_grad(to):
        t = got_x(2 * to + y)
        remote(y_send.at[to], y_recv.at[to], y_s.at[to], y_r.at[to], y_peer).wait_recv()
        return t + y_recv[to].astype(f32)

    def grad_z(to):
        z_send[to] = got_grad(to).astype(jnp.bfloat16)
        send(z_send.at[to], z_recv.at[z], z_s.at[to], z_r.at[z], z_peer(to))

    core_f.wait_recv()
    early = order[:owners]
    for to in early:
        factor_y(to)
    core_c.wait_recv()
    for to in early:
        grad_y(to)
    for to in early:
        factor_z(to)
    late = order[owners:]
    for to in late:
        grad_y(to)
    for to in late:
        factor_y(to)
    for to in early:
        grad_z(to)
    for to in late[:-1]:
        grad_z(to)
    gc_send[...] = got_grad(z)
    for to in late[:-1]:
        factor_z(to)
    f_total = got_factor(z)

    def z_sum(sends, recvs, s, r, total):
        for src in order[:-1]:
            remote(sends.at[src], recvs.at[src], s.at[src], r.at[src], z_peer(src)).wait_recv()
            total = total + recvs[src].astype(f32)
        return total

    block = x * per_x + seq
    b, m = block // out_blocks, block % out_blocks
    loads[2].wait()
    loads[3].wait()

    def pick(ref, which, count):
        part = ref[:, :BLOCK]
        for n in range(1, count):
            part = jnp.where(which == n, ref[:, n * BLOCK:(n + 1) * BLOCK], part)
        return part

    p_t = pick(pinv_ref, b, in_blocks)
    q_t = pick(qinv_ref, m, out_blocks)
    q_tail = jnp.concatenate([q_t[LANE:], jnp.zeros((PAD - BLOCK, BLOCK), f32)], axis=0)
    q_half = jnp.where(first, q_t[:LANE], q_tail)
    p_now = p_t.T

    gc_send[...] = z_sum(z_send, z_recv, z_s, z_r, gc_send[...])
    fin_g = send(gc_send, gc_recv, fin_s.at[1], fin_r.at[1], core_peer)
    fin_g.wait_recv()
    ours, theirs = gc_send[...], gc_recv[...]
    left = jnp.where(first, ours, theirs)[:BLOCK]
    right = jnp.where(first, theirs, ours)[:BLOCK]
    full = jnp.concatenate([left, right[:, :BLOCK - LANE]], axis=1) * scale
    right_done = lax.dot_general(
        full, q_half, (((1,), (1,)), ((), ())), precision=lax.Precision.HIGHEST, preferred_element_type=f32
    )
    applied = jnp.dot(p_now, right_done, precision=lax.Precision.HIGHEST, preferred_element_type=f32)
    applied = jnp.concatenate([applied, jnp.zeros((rows - BLOCK, LANE), f32)], axis=0)
    ag[c, block] = applied.astype(jnp.bfloat16)

    def gather(g, s, r, peer):
        return remote(ag.at[c, g], ag.at[c, g], s, r, peer)

    def start(copy):
        copy.start()
        pending.append(copy)

    base, away = x * per_x, (1 - x) * per_x
    for to in order[:-1]:
        start(gather(block, az_s.at[to], az_r.at[z], z_peer(to)))

    def on_y(g, slot):
        start(gather(g, ay_s.at[slot], ay_r.at[slot], y_peer))

    def on_x(k):
        start(gather(base + k, ax_s.at[k], ax_r.at[k], x_peer))

    def on_core(g):
        start(gather(g, ac_s.at[g], ac_r.at[g], core_peer))

    def arrived_y(i):
        zz = around(i)
        k = 2 * zz + 1 - y
        gather(base + k, ay_s.at[zz], ay_r.at[zz], y_peer).wait_recv()
        on_x(k)
        on_core(base + k)

    def arrived_x(i):
        zz = around(i)
        k = 2 * zz + y
        gather(away + k, ax_s.at[k], ax_r.at[k], x_peer).wait_recv()
        on_core(away + k)

    def arrived_far(i):
        zz = around(i)
        k = 2 * zz + 1 - y
        gather(away + k, ax_s.at[k], ax_r.at[k], x_peer).wait_recv()
        on_core(away + k)

    on_x(seq)
    on_y(block, z)
    on_core(block)

    f_total = z_sum(fz_send, fz_recv, fz_s, fz_r, f_total)
    fx_send[...] = f_total.astype(jnp.bfloat16)
    fin_x = send(fx_send, fx_recv, fin_s.at[0], fin_r.at[0], x_peer)

    for i in range(1, near):
        src = around(i)
        k = 2 * src + y
        gather(base + k, az_s.at[src], az_r.at[src], z_peer(src)).wait_recv()
        on_y(base + k, src)
        on_x(k)
        on_core(base + k)
        arrived_y(i - 1)
        arrived_x(i - 1)

    fin_x.wait_recv()
    fc_send[...] = fx_send[...].astype(f32) + fx_recv[...].astype(f32)
    fin_c = send(fc_send, fc_recv, fin_s.at[2], fin_r.at[2], core_peer)
    arrived_y(near - 1)
    arrived_x(near - 1)

    fin_c.wait_recv()
    take = fx_ref.shape[1]
    skip = take - step
    for j, ref in enumerate((fx_ref, fy_ref)):
        ours, theirs = fc_send[j], fc_recv[j]
        left = jnp.where(first, ours, theirs)
        right = jnp.where(first, theirs, ours)
        both = jnp.concatenate([left, right[:, :BLOCK - LANE]], axis=1) * scale
        ref[...] = jnp.where(y == 0, both[:take], both[skip:skip + take]).T

    for i in range(near):
        arrived_far(i)
    for g in range(2 * per_x):
        remote(ag.at[1 - c, g], ag.at[1 - c, g], ac_s.at[g], ac_r.at[g], core_peer).wait_recv()

    for pair in range(in_blocks // 2):
        strips = []
        for bi in (2 * pair, 2 * pair + 1):
            parts = []
            for mi in range(out_blocks):
                g = bi * out_blocks + mi
                parts.append(ag[0, g].astype(f32)[:BLOCK])
                parts.append(ag[1, g].astype(f32)[:BLOCK, :BLOCK - LANE])
            strips.append(jnp.concatenate(parts, axis=1))
        whole = jnp.concatenate(strips, axis=0).astype(jnp.bfloat16)
        out_ref[2 * pair * BLOCK:2 * (pair + 1) * BLOCK, :] = whole
    for copy in pending:
        copy.wait_send()


def fused(layer_inputs, output_grads, input_inverse, output_inverse):
    tok, in_width = layer_inputs.shape
    out_width = output_grads.shape[1]
    in_blocks, out_blocks = in_width // BLOCK, out_width // BLOCK
    seq = lax.axis_size("seq")
    near = seq // 2
    rows = round_up(BLOCK, 16)
    take = in_width // seq
    step = take // 16 * 16
    window = rows - step
    blocks = in_blocks * out_blocks
    per_x = blocks // 2
    bf16, f32 = jnp.bfloat16, jnp.float32
    vmem = pltpu.VMEM
    dma = pltpu.SemaphoreType.DMA
    g = (rows, LANE)
    f = (2, window, LANE)
    hbm = pl.BlockSpec(memory_space=pltpu.HBM)
    scratch = [
        vmem(layer_inputs.shape, bf16),
        vmem(output_grads.shape, bf16),
        vmem((BLOCK, in_width), f32),
        vmem((BLOCK, out_width), f32),
        dma((4,)),
        vmem((tok, in_blocks * PAD), bf16),
        vmem((tok, out_blocks * PAD), bf16),
        vmem((per_x, *g), f32),
        vmem((per_x, *g), f32),
        vmem((blocks, *g), bf16),
        vmem((blocks, *g), bf16),
        vmem((per_x, *g), bf16),
        vmem((per_x, *g), bf16),
        vmem((near, *g), bf16),
        vmem((near, *g), bf16),
        vmem((near, *g), bf16),
        vmem((near, *g), bf16),
        vmem((seq, *f), f32),
        vmem((seq, *f), bf16),
        vmem((seq, *f), bf16),
        vmem((near, *f), bf16),
        vmem((near, *f), bf16),
        vmem((near, *f), bf16),
        vmem((near, *f), bf16),
        vmem(f, bf16),
        vmem(f, bf16),
        vmem(f, f32),
        vmem(f, f32),
        vmem(g, f32),
        vmem(g, f32),
        vmem((2, blocks, *g), bf16),
    ]
    for count in (4, per_x, near, near, near, near, 3, near, 2 * near, per_x, blocks):
        scratch += [dma((count,)), dma((count,))]
    fx, fy, out = pl.pallas_call(
        functools.partial(kernel, near),
        out_shape=(
            pltpu.VMEM((BLOCK, take), f32),
            pltpu.VMEM((BLOCK, out_width // seq), f32),
            pltpu.VMEM((in_width, out_width), bf16),
        ),
        in_specs=[hbm] * 4,
        out_specs=(pl.BlockSpec(memory_space=vmem),) * 3,
        scratch_shapes=scratch,
        compiler_params=pltpu.CompilerParams(
            collective_id=0, has_side_effects=True, vmem_limit_bytes=62000000
        ),
    )(layer_inputs, output_grads, input_inverse.T, output_inverse.T)
    fx, fy, out = settle(fx, fy, out)
    return fx.T, fy.T, out


def settle_kernel(a, b, c, a_out, b_out, c_out, sems):
    copies = [
        pltpu.make_async_copy(src, dst, sems.at[i])
        for i, (src, dst) in enumerate(((a, a_out), (b, b_out), (c, c_out)))
    ]
    for copy in copies:
        copy.start()
    for copy in copies:
        copy.wait()


def settle(*arrays):
    return pl.pallas_call(
        settle_kernel,
        out_shape=tuple(jax.ShapeDtypeStruct(a.shape, a.dtype) for a in arrays),
        in_specs=[pl.BlockSpec(memory_space=pltpu.VMEM)] * 3,
        out_specs=(pl.BlockSpec(memory_space=pltpu.HBM),) * 3,
        scratch_shapes=[pltpu.SemaphoreType.DMA((3,))],
        compiler_params=pltpu.CompilerParams(vmem_limit_bytes=4 * 2**20),
    )(*arrays)


def solution(mesh):
    def step(layer_inputs, output_grads, input_inverse, output_inverse):
        in_width, out_width = layer_inputs.shape[1], output_grads.shape[1]
        in_blocks, out_blocks = in_width // BLOCK, out_width // BLOCK
        fits = (
            mesh.shape["batch"] == 4
            and in_blocks * out_blocks == 2 * mesh.shape["seq"]
            and in_blocks == out_blocks
            and 2 * in_blocks == mesh.shape["seq"]
            and in_blocks // 2 == 2
        )
        body = fused if fits else shards
        return body(layer_inputs, output_grads, input_inverse, output_inverse)

    return jax.shard_map(
        step,
        mesh=mesh,
        in_specs=(P(("batch", "seq"), None), P(("batch", "seq"), None), P(), P()),
        out_specs=(P("seq", None), P("seq", None), P()),
        check_vma=False,
    )
```

```python
import functools

import jax
import jax.numpy as jnp
from jax import lax
from jax.experimental import pallas as pl
from jax.experimental.pallas import tpu as pltpu
from jax.sharding import PartitionSpec as P

BLOCK = 200


def block_terms(values):
    tok_rows, width = values.shape
    stacked = values.reshape(tok_rows, width // BLOCK, BLOCK)
    product = jnp.einsum("tnb,tnc->nbc", stacked, stacked, preferred_element_type=jnp.float32)
    return product.reshape(width, BLOCK)


def reduce_terms(input_term, output_term, grad_term):
    shares = (
        lax.psum_scatter(
            input_term.astype(jnp.bfloat16), "seq", scatter_dimension=0, tiled=True
        ).astype(jnp.float32),
        lax.psum_scatter(
            output_term.astype(jnp.bfloat16), "seq", scatter_dimension=0, tiled=True
        ).astype(jnp.float32),
        lax.psum_scatter(
            grad_term.astype(jnp.bfloat16), "seq", scatter_dimension=0, tiled=True
        ).astype(jnp.float32),
    )
    return lax.psum((shares[0], shares[1], shares[2]), "batch")


def shards(layer_inputs, output_grads, input_inverse, output_inverse):
    tok_rows, in_width = layer_inputs.shape
    out_width = output_grads.shape[1]
    in_blocks = in_width // BLOCK
    out_blocks = out_width // BLOCK
    total_rows = tok_rows * lax.axis_size("batch") * lax.axis_size("seq")
    inverse_count = 1.0 / total_rows
    input_term = block_terms(layer_inputs)
    output_term = block_terms(output_grads)
    input_stack = input_inverse.reshape(in_blocks, BLOCK, BLOCK)
    output_stack = output_inverse.reshape(out_blocks, BLOCK, BLOCK)
    grad_term = lax.dot_general(
        layer_inputs, output_grads, (((0,), (0,)), ((), ())), preferred_element_type=jnp.float32
    )
    input_sum, output_sum, grad_sum = reduce_terms(input_term, output_term, grad_term)
    grad_owned = grad_sum * inverse_count
    owned_rows = grad_owned.shape[0]
    right_done = jnp.einsum(
        "rmk,mkl->rml",
        grad_owned.reshape(owned_rows, out_blocks, BLOCK),
        output_stack,
        precision=lax.Precision.HIGHEST,
    ).reshape(owned_rows, out_width)
    gathered = lax.all_gather(right_done, "seq", axis=0, tiled=True)
    applied = jnp.einsum(
        "nij,njo->nio",
        input_stack,
        gathered.reshape(in_blocks, BLOCK, out_width),
        precision=lax.Precision.HIGHEST,
    ).reshape(in_width, out_width)
    preconditioned = applied.astype(jnp.bfloat16)
    input_factor = input_sum * inverse_count
    output_factor = output_sum * inverse_count
    return (input_factor, output_factor, preconditioned)


LANE = 128
PAD = 2 * LANE
MESH = pl.DeviceIdType.MESH


def round_up(size, unit):
    return (size + unit - 1) // unit * unit


def kernel(
    near, x_hbm, y_hbm, pinv_hbm, qinv_hbm, fx_ref, fy_ref, out_ref,
    x_ref, y_ref, pinv_ref, qinv_ref, load_s, xp, yp, xq, yq, own, stage, core,
    x_send, x_recv, y_send, y_recv, z_send, z_recv,
    f_own, f_stage, f_core, fy_send, fy_recv, fz_send, fz_recv, fx_send, fx_recv, fc_send, fc_recv, ag,
    core_s, core_r, x_s, x_r, y_s, y_r, z_s, z_r, fy_s, fy_r, fz_s, fz_r, fin_s, fin_r,
    az_s, az_r, ay_s, ay_r, ax_s, ax_r, ac_s, ac_r,
):
    batch, seq = lax.axis_index("batch"), lax.axis_index("seq")
    x, c = batch // 2, batch % 2
    z, y = seq // 2, seq % 2
    tok, in_width = x_hbm.shape
    out_width = y_hbm.shape[1]
    in_blocks, out_blocks = in_width // BLOCK, out_width // BLOCK
    strip = own.shape[2]
    tiles = near - 1
    whole = 2 * tiles * LANE
    rest = out_width - whole
    mid = in_width // strip // 2
    window, step = f_own.shape[2], round_up(BLOCK, 16) - f_own.shape[2]
    scale = 1.0 / (tok * lax.axis_size("batch") * lax.axis_size("seq"))
    core_peer = (2 * x + 1 - c, seq)
    x_peer = (2 * (1 - x) + c, seq)
    y_peer = (batch, 2 * z + 1 - y)
    f32, bf16 = jnp.float32, jnp.bfloat16
    first = c == 0

    def z_peer(to):
        return (batch, 2 * to + y)

    by_distance = [z + 1 - 2 * (z % 2), 2 - z // 2, 3 * (1 - z // 2)]
    others = by_distance[::-1]

    def remote(src, dst, s, r, peer):
        return pltpu.make_async_remote_copy(
            src_ref=src, dst_ref=dst, send_sem=s, recv_sem=r, device_id=peer, device_id_type=MESH
        )

    pending = []

    def send(*args):
        copy = remote(*args)
        copy.start()
        pending.append(copy)
        return copy

    loads = [
        pltpu.make_async_copy(src, dst, load_s.at[i])
        for i, (src, dst) in enumerate(
            ((x_hbm, x_ref), (pinv_hbm, pinv_ref), (y_hbm, y_ref), (qinv_hbm, qinv_ref))
        )
    ]
    for load in loads:
        load.start()
    barrier = pltpu.get_barrier_semaphore()
    peers = [core_peer, x_peer, y_peer] + [z_peer(to) for to in others]
    for peer in peers:
        pl.semaphore_signal(barrier, inc=1, device_id=peer, device_id_type=MESH)

    def padded(ref, out, blocks):
        for b in range(blocks):
            part = ref[:, b * BLOCK:(b + 1) * BLOCK]
            out[:, b * PAD:b * PAD + BLOCK] = part
            out[:, b * PAD + BLOCK:(b + 1) * PAD] = jnp.zeros((tok, PAD - BLOCK), out.dtype)

    def two_terms(v):
        high = v.astype(bf16)
        low = (v - high.astype(f32)).astype(bf16)
        return jnp.concatenate([high, low], axis=1)

    def last_dims(a, b):
        return lax.dot_general(a, b, (((1,), (1,)), ((), ())), preferred_element_type=f32)

    def tdot(a, b):
        return lax.dot_general(a, b, (((0,), (0,)), ((), ())), preferred_element_type=f32)

    def twice(v):
        return jnp.concatenate([v, v], axis=1)

    fill = PAD - BLOCK
    loads[0].wait()
    padded(x_ref, xp, in_blocks)
    loads[1].wait()
    for b in range(in_blocks):
        p_t = pinv_ref[:, b * BLOCK:(b + 1) * BLOCK]
        p = jnp.concatenate([p_t, jnp.zeros((fill, BLOCK), f32)], axis=0).T
        part = last_dims(two_terms(p), twice(xp[:, b * PAD:(b + 1) * PAD]))
        xq[b * BLOCK:(b + 1) * BLOCK, :] = part.astype(bf16)
    loads[2].wait()
    padded(y_ref, yp, out_blocks)
    loads[3].wait()
    for m in range(out_blocks):
        q_t = qinv_ref[:, m * BLOCK:(m + 1) * BLOCK]
        q_t = jnp.concatenate([q_t, jnp.zeros((BLOCK, fill), f32)], axis=1)
        part = last_dims(twice(yp[:, m * PAD:(m + 1) * PAD]), two_terms(q_t))
        yq[:, m * BLOCK:(m + 1) * BLOCK] = part.astype(bf16)
    yq[:, out_width:] = jnp.zeros((tok, yq.shape[1] - out_width), bf16)

    def keep(group, k, left, right):
        own[group, k] = jnp.where(first, left, right)
        stage[group, k] = jnp.where(first, right, left).astype(bf16)

    def product(row):
        rows = pl.ds(pl.multiple_of(strip * row, strip), strip)
        return jnp.dot(xq[rows, :], yq[:, :whole], preferred_element_type=f32)

    def tile(v, t):
        return v[:, t * LANE:(t + 1) * LANE]

    def strips(to_x, to_y):
        row = to_x * (2 * mid - 2 * to_y) + to_y
        v = product(row)
        for t in range(tiles):
            keep(2 * to_x + to_y, t, tile(v, t), tile(v, tiles + t))

    def middle():
        v = product(mid)
        for t in range(tiles):
            keep(t, tiles, tile(v, t), tile(v, tiles + t))
        tail = jnp.dot(xq[...], yq[:, whole:], preferred_element_type=f32)
        folded = tail[:BLOCK]
        for b in range(1, in_blocks):
            folded = folded + pltpu.roll(tail[b * BLOCK:(b + 1) * BLOCK], b * rest, 1)
        skip = BLOCK // 16 * 8
        take = BLOCK - skip
        none = jnp.zeros((strip - take, LANE), f32)
        keep(tiles, tiles, jnp.concatenate([folded[:take], none], axis=0), jnp.concatenate([folded[skip:], none], axis=0))

    def swap(at, i):
        return send(stage.at[at], core.at[at], core_s.at[i], core_r.at[i], core_peer)

    far_far, far_own = 2 * (1 - x) + 1 - y, 2 * (1 - x) + y
    strips(1 - x, 1 - y)
    pl.semaphore_wait(barrier, len(peers))
    core_a = swap((far_far, pl.ds(0, tiles)), 0)
    strips(1 - x, y)
    core_b = swap((far_own, pl.ds(0, tiles)), 1)

    def on_chip(group, k):
        return own[group, k] + core[group, k].astype(f32)

    def to_x(yy, k):
        x_send[yy, k] = on_chip(2 * (1 - x) + yy, k).astype(bf16)
        i = near * yy + k
        send(x_send.at[yy, k], x_recv.at[yy, k], x_s.at[i], x_r.at[i], x_peer)

    core_a.wait_recv()
    for k in range(tiles):
        to_x(1 - y, k)
    middle()
    core_c = swap((pl.ds(0, 4), tiles), 2)
    core_b.wait_recv()
    core_c.wait_recv()
    to_x(1 - y, tiles)
    for k in others + [z]:
        to_x(y, k)

    def mine(v):
        return jnp.where(first, v[:, :LANE], v[:, LANE:PAD])

    def other(v):
        return jnp.where(first, v[:, LANE:PAD], v[:, :LANE])

    def factors(j, src):
        for b in range(in_blocks):
            part = src[:, b * PAD:(b + 1) * PAD]
            prod = tdot(part, part)
            kept, away = mine(prod), other(prod)
            for h in range(2):
                f_own[2 * b + h, j] = kept[h * step:h * step + window]
                f_stage[2 * b + h, j] = away[h * step:h * step + window].astype(bf16)

    factors(0, xp)
    factors(1, yp)
    core_f = send(f_stage, f_core, core_s.at[3], core_r.at[3], core_peer)
    strips(x, 1 - y)
    strips(x, y)
    core_d = swap((pl.ds(2 * x, 2), pl.ds(0, tiles)), 4)

    def got_x(yy, k):
        i = near * yy + k
        remote(x_send.at[yy, k], x_recv.at[yy, k], x_s.at[i], x_r.at[i], x_peer).wait_recv()
        return on_chip(2 * x + yy, k) + x_recv[yy, k].astype(f32)

    def grad_y(to):
        y_send[to] = got_x(1 - y, to).astype(bf16)
        send(y_send.at[to], y_recv.at[to], y_s.at[to], y_r.at[to], y_peer)

    def factor_y(to):
        k = 2 * to + 1 - y
        fy_send[to] = (f_own[k] + f_core[k].astype(f32)).astype(bf16)
        send(fy_send.at[to], fy_recv.at[to], fy_s.at[to], fy_r.at[to], y_peer)

    def got_factor(to):
        k = 2 * to + y
        remote(fy_send.at[to], fy_recv.at[to], fy_s.at[to], fy_r.at[to], y_peer).wait_recv()
        return f_own[k] + f_core[k].astype(f32) + fy_recv[to].astype(f32)

    def factor_z(to):
        fz_send[to] = got_factor(to).astype(bf16)
        send(fz_send.at[to], fz_recv.at[z], fz_s.at[to], fz_r.at[z], z_peer(to))

    def got_grad(to):
        total = got_x(y, to)
        remote(y_send.at[to], y_recv.at[to], y_s.at[to], y_r.at[to], y_peer).wait_recv()
        return total + y_recv[to].astype(f32)

    def grad_z(to):
        z_send[to] = got_grad(to).astype(bf16)
        send(z_send.at[to], z_recv.at[z], z_s.at[to], z_r.at[z], z_peer(to))

    core_f.wait_recv()
    for to in others[:2]:
        factor_y(to)
    core_d.wait_recv()
    grad_y(0)
    grad_y(1)
    for to in others[:2]:
        factor_z(to)
    grad_y(2)
    factor_y(others[2])
    grad_y(3)
    factor_y(z)
    for to in others:
        grad_z(to)
    factor_z(others[2])
    g_total = got_grad(z)
    f_total = got_factor(z)

    def z_sum(sends, recvs, s, r, total):
        for src in by_distance:
            remote(sends.at[src], recvs.at[src], s.at[src], r.at[src], z_peer(src)).wait_recv()
            total = total + recvs[src].astype(f32)
        return total

    here = 2 * x + y
    ag[c, here, z] = (z_sum(z_send, z_recv, z_s, z_r, g_total) * scale).astype(bf16)

    def gather(group, k, s, r, peer):
        return remote(ag.at[c, group, k], ag.at[c, group, k], s, r, peer)

    def start(copy):
        copy.start()
        pending.append(copy)

    by_x, by_y, across = 2 * (1 - x) + y, 2 * x + 1 - y, 2 * (1 - x) + 1 - y

    def on_core(group, k):
        i = near * group + k
        start(gather(group, k, ac_s.at[i], ac_r.at[i], core_peer))

    def spread(k):
        start(gather(here, k, ay_s.at[k], ay_r.at[k], y_peer))
        start(gather(here, k, ax_s.at[k], ax_r.at[k], x_peer))
        on_core(here, k)

    def arrived_z(src):
        gather(here, src, az_s.at[src], az_r.at[src], z_peer(src)).wait_recv()
        spread(src)

    def arrived_x(k, forward):
        gather(by_x, k, ax_s.at[k], ax_r.at[k], x_peer).wait_recv()
        if forward:
            start(gather(by_x, k, ay_s.at[near + k], ay_r.at[near + k], y_peer))
        on_core(by_x, k)

    def arrived_y(k, forward):
        gather(by_y, k, ay_s.at[k], ay_r.at[k], y_peer).wait_recv()
        if forward:
            start(gather(by_y, k, ax_s.at[near + k], ax_r.at[near + k], x_peer))
        on_core(by_y, k)

    def arrived_across(k, on_y):
        if on_y:
            gather(across, k, ay_s.at[near + k], ay_r.at[near + k], y_peer).wait_recv()
        else:
            gather(across, k, ax_s.at[near + k], ax_r.at[near + k], x_peer).wait_recv()
        on_core(across, k)

    for to in others:
        start(gather(here, z, az_s.at[to], az_r.at[z], z_peer(to)))
    spread(z)

    f_total = z_sum(fz_send, fz_recv, fz_s, fz_r, f_total)
    fx_send[...] = f_total.astype(bf16)
    fin_x = send(fx_send, fx_recv, fin_s.at[0], fin_r.at[0], x_peer)

    arrival = [z] + by_distance
    for i in range(1, near):
        arrived_z(arrival[i])
        arrived_x(arrival[i - 1], i % 2 == 1)
        arrived_y(arrival[i - 1], i % 2 == 0)
    fin_x.wait_recv()
    fc_send[...] = fx_send[...].astype(f32) + fx_recv[...].astype(f32)
    fin_c = send(fc_send, fc_recv, fin_s.at[1], fin_r.at[1], core_peer)
    arrived_x(arrival[-1], False)
    arrived_y(arrival[-1], True)
    for i in range(near):
        arrived_across(arrival[i], i % 2 == 0)

    fin_c.wait_recv()
    take = fx_ref.shape[1]
    skip = take - step
    for j, ref in enumerate((fx_ref, fy_ref)):
        ours, theirs = fc_send[j], fc_recv[j]
        left = jnp.where(first, ours, theirs)
        right = jnp.where(first, theirs, ours)
        both = jnp.concatenate([left, right[:, :BLOCK - LANE]], axis=1) * scale
        ref[...] = jnp.where(y == 0, both[:take], both[skip:skip + take]).T

    def place(half, group, k):
        if k < tiles:
            row, t = (group // 2) * (2 * mid - 2 * (group % 2)) + group % 2, k
        else:
            row, t = mid, group
        lanes = pl.ds(pl.multiple_of((half * tiles + t) * LANE, LANE), LANE)
        out_ref[row * strip:(row + 1) * strip, lanes] = ag[half, group, k]

    pieces = [(group, k) for group in range(4) for k in range(near)]
    for group, k in pieces[:-1]:
        place(c, group, k)
    for group, k in pieces:
        i = near * group + k
        remote(ag.at[1 - c, group, k], ag.at[1 - c, group, k], ac_s.at[i], ac_r.at[i], core_peer).wait_recv()
        if i < len(pieces) - 1:
            place(1 - c, group, k)
    skip = BLOCK // 16 * 8
    folded = jnp.concatenate(
        [ag[0, tiles, tiles].astype(f32)[:skip], ag[1, tiles, tiles].astype(f32)[:BLOCK - skip]], axis=0
    )
    parts = [folded if b == 0 else pltpu.roll(folded, LANE - b * rest, 1) for b in range(in_blocks)]
    out_ref[:, whole:] = jnp.concatenate(parts, axis=0)[:, :rest].astype(bf16)
    for copy in pending:
        copy.wait_send()


def fused(layer_inputs, output_grads, input_inverse, output_inverse):
    tok, in_width = layer_inputs.shape
    out_width = output_grads.shape[1]
    in_blocks, out_blocks = in_width // BLOCK, out_width // BLOCK
    seq = lax.axis_size("seq")
    near = seq // 2
    take = in_width // seq
    step = take // 16 * 16
    window = round_up(BLOCK, 16) - step
    strip = in_width // (near + 1)
    bf16, f32 = jnp.bfloat16, jnp.float32
    vmem = pltpu.VMEM
    dma = pltpu.SemaphoreType.DMA
    g = (strip, LANE)
    f = (2, window, LANE)
    hbm = pl.BlockSpec(memory_space=pltpu.HBM)
    scratch = [
        vmem(layer_inputs.shape, bf16),
        vmem(output_grads.shape, bf16),
        vmem((BLOCK, in_width), f32),
        vmem((BLOCK, out_width), f32),
        dma((4,)),
        vmem((tok, in_blocks * PAD), bf16),
        vmem((tok, out_blocks * PAD), bf16),
        vmem((in_width, tok), bf16),
        vmem((tok, round_up(out_width, LANE)), bf16),
        vmem((4, near, *g), f32),
        vmem((4, near, *g), bf16),
        vmem((4, near, *g), bf16),
        vmem((2, near, *g), bf16),
        vmem((2, near, *g), bf16),
        vmem((near, *g), bf16),
        vmem((near, *g), bf16),
        vmem((near, *g), bf16),
        vmem((near, *g), bf16),
        vmem((seq, *f), f32),
        vmem((seq, *f), bf16),
        vmem((seq, *f), bf16),
        vmem((near, *f), bf16),
        vmem((near, *f), bf16),
        vmem((near, *f), bf16),
        vmem((near, *f), bf16),
        vmem(f, bf16),
        vmem(f, bf16),
        vmem(f, f32),
        vmem(f, f32),
        vmem((2, 4, near, *g), bf16),
    ]
    for count in (5, 2 * near, near, near, near, near, 2, near, 2 * near, 2 * near, 4 * near):
        scratch += [dma((count,)), dma((count,))]
    results = pl.pallas_call(
        functools.partial(kernel, near),
        out_shape=(
            vmem((BLOCK, take), f32),
            vmem((BLOCK, out_width // seq), f32),
            vmem((in_width, out_width), bf16),
        ),
        in_specs=[hbm] * 4,
        out_specs=(pl.BlockSpec(memory_space=vmem),) * 3,
        scratch_shapes=scratch,
        compiler_params=pltpu.CompilerParams(
            collective_id=0, has_side_effects=True, vmem_limit_bytes=62000000
        ),
    )(layer_inputs, output_grads, input_inverse.T, output_inverse.T)
    fx, fy, out = settle(*results)
    return fx.T, fy.T, out


def settle_kernel(a, b, c, a_out, b_out, c_out, sems):
    copies = [
        pltpu.make_async_copy(src, dst, sems.at[i])
        for i, (src, dst) in enumerate(((a, a_out), (b, b_out), (c, c_out)))
    ]
    for copy in copies:
        copy.start()
    for copy in copies:
        copy.wait()


def settle(*arrays):
    return pl.pallas_call(
        settle_kernel,
        out_shape=tuple(jax.ShapeDtypeStruct(a.shape, a.dtype) for a in arrays),
        in_specs=[pl.BlockSpec(memory_space=pltpu.VMEM)] * 3,
        out_specs=(pl.BlockSpec(memory_space=pltpu.HBM),) * 3,
        scratch_shapes=[pltpu.SemaphoreType.DMA((3,))],
        compiler_params=pltpu.CompilerParams(vmem_limit_bytes=4 * 2**20),
    )(*arrays)


def solution(mesh):
    def step(layer_inputs, output_grads, input_inverse, output_inverse):
        in_width, out_width = layer_inputs.shape[1], output_grads.shape[1]
        blocks = in_width // BLOCK
        near = mesh.shape["seq"] // 2
        rest = out_width % LANE
        fits = (
            mesh.shape["batch"] == 4
            and near == 4
            and blocks == near
            and in_width == out_width == blocks * BLOCK
            and out_width // LANE == 2 * (near - 1)
            and in_width % (16 * (near + 1)) == 0
            and rest * blocks == LANE
        )
        body = fused if fits else shards
        return body(layer_inputs, output_grads, input_inverse, output_inverse)

    return jax.shard_map(
        step,
        mesh=mesh,
        in_specs=(P(("batch", "seq"), None), P(("batch", "seq"), None), P(), P()),
        out_specs=(P("seq", None), P("seq", None), P()),
        check_vma=False,
    )
```
